32 devices in a mesh: dp: 8 (over z, core), row: 2 (over y), col: 2 (over x).
Axes of the slice: x: 2, y: 2, z: 4, core: 2. Of those that a mesh axis runs over, the one named last changes fastest.
Arguments:
- patches: bfloat16 [4096, 1408], P(('dp', 'row', 'col')), may hold values from -6 to 6
- norm_gain: float32 [1408], replicated, may hold values from 0.5 to 1.5
- norm_bias: float32 [1408], replicated, may hold values from -3 to 3
- up_weight: bfloat16 [1408, 6144], P('col', 'row'), may hold values from -0.15625 to 0.15625
- up_bias: float32 [6144], P('row'), may hold values from -3 to 3
- down_weight: bfloat16 [6144, 1408], P('row', 'col'), may hold values from -0.078125 to 0.078125
- down_bias: float32 [1408], replicated, may hold values from -3 to 3
- cotangent: bfloat16 [4096, 1408], P(('dp', 'row', 'col')), may hold values from -6 to 6
Outputs:
- output: float32 [4096, 1408], P(('dp', 'row', 'col'))
- patch_grad: float32 [4096, 1408], P(('dp', 'row', 'col'))
- up_grad: float32 [1408, 6144], P('col', 'row')
- down_grad: float32 [6144, 1408], P('row', 'col')
- bias_grad: float32 [6144], P('row')
- norm_grad: float32 [2, 1408], replicated
The draws below stay inside these ranges and needn't reach their ends.
All inputs are finite; a program needn't handle non-finite values.
Results may differ from the reference program's by a relative error of at most 0.0055.
Values may be sent and summed in bfloat16 or wider, within the bound.
A program may use at most 128 MiB of HBM per device.

```python
import math
import jax
import jax.numpy as jnp
from jax import lax

D = 1408
FF = 6144
TOK_DEV = 128
TOKENS = 4096
N_DP = 8
N_ROW = 2
N_COL = 2


def spiked(drawn, own_key, source, target, shards_of, factor):
    owner, partner = [(jnp.arange(drawn.shape[dim]) // (drawn.shape[dim] // shards_of)).reshape([-1 if axis == dim else 1 for axis in range(drawn.ndim)]) for dim in (source, target)]
    chosen = jax.random.permutation(own_key, shards_of)[partner]
    strong = (owner == chosen) | (owner == (partner + shards_of // 2) % shards_of)
    return jnp.where(strong, factor * drawn, drawn)


def block_levels(key, dims, split, smallest, largest):
    def one(axis_at, parts):
        steps = jax.random.uniform(jax.random.fold_in(jax.random.fold_in(key, 6), axis_at), (parts,), jnp.float32, smallest / len(split), largest / len(split))
        return jnp.repeat(jnp.exp(steps), dims[axis_at] // parts).reshape((-1,) + (1,) * (len(dims) - axis_at - 1))

    loudness = one(*split[0])
    for cut in split[1:]:
        loudness = loudness * one(*cut)
    return loudness


def noise(stream_key, shape, deviation, most, shards=(), kind=jnp.bfloat16):
    factor_of = block_levels(stream_key, shape, shards, -0.22, 0.18) if shards else 1.0
    result = jax.random.normal(stream_key, shape, jnp.float32) * deviation * factor_of
    return jnp.minimum(jnp.maximum(result, -most), most).astype(kind)


def noise_with(rng, dims, scale, reach, split, heavy, dtype=jnp.bfloat16):
    drawn = scale * jax.random.normal(rng, dims, jnp.float32)
    if split:
        drawn = drawn * block_levels(rng, dims, split, -0.22, 0.18)
    return jnp.clip(spiked(drawn, jax.random.fold_in(rng, 3), *heavy), -reach, reach).astype(dtype)


def setup_inputs(seed: int = 0) -> dict:
    arg_keys = jax.random.split(jax.random.key(seed), 9)
    return {
        "patches": noise(arg_keys[0], (TOKENS, D), 1.0, 6.0, ((0, 32),)),
        "norm_gain": jnp.clip(1.0 + 0.1 * jax.random.normal(arg_keys[1], (D,), jnp.float32), 0.5, 1.5),
        "norm_bias": noise(arg_keys[2], (D,), 0.5, 3.0, (), jnp.float32),
        "up_weight": noise(arg_keys[3], (D, FF), D ** -0.5, 0.15625, ((0, 2), (1, 2))),
        "up_bias": noise(arg_keys[4], (FF,), 0.5, 3.0, ((0, 2),), jnp.float32),
        "down_weight": noise(arg_keys[5], (FF, D), FF ** -0.5, 0.078125, ((0, 2), (1, 2))),
        "down_bias": noise(arg_keys[6], (D,), 0.5, 3.0, (), jnp.float32),
        "cotangent": noise_with(arg_keys[7], (TOKENS, D), 1.0, 6.0, ((0, 32),), (0, 1, 32, 2.75)),
    }


EPSILON = 1e-06
GELU_ROOT = 0.7978845608028654
GELU_CUBIC = 0.044715

def gelu_value(value):
    inner = jnp.tanh(GELU_ROOT * (value + GELU_CUBIC * value * value * value))
    return 0.5 * value * (1.0 + inner)

def gelu_slope(value):
    inner = jnp.tanh(GELU_ROOT * (value + GELU_CUBIC * value * value * value))
    return 0.5 * (1.0 + inner) + 0.5 * value * (1.0 - inner * inner) * GELU_ROOT * (1.0 + 3.0 * GELU_CUBIC * value * value)

def reference(patches, norm_gain, norm_bias, up_weight, up_bias, down_weight, down_bias, cotangent):
    replica_rows = TOK_DEV * N_ROW * N_COL
    patch_blocks = patches.reshape(N_DP, replica_rows, D)
    upstream_blocks = cotangent.reshape(N_DP, replica_rows, D)

    def one_block(carry, pieces):
        up_acc, down_acc, bias_acc, gain_acc, shift_acc = carry
        block, upstream = pieces
        wide = block.astype(jnp.float32)
        centred = wide - lax.optimization_barrier(jnp.mean(wide, axis=1, keepdims=True))
        inverse_spread = lax.rsqrt(lax.optimization_barrier(jnp.mean(centred * centred, axis=1, keepdims=True)) + EPSILON)
        standard = centred * inverse_spread
        normed = (standard * norm_gain + norm_bias).astype(jnp.bfloat16)
        preact = jnp.dot(normed, up_weight, preferred_element_type=jnp.float32) + up_bias
        activated = gelu_value(preact).astype(jnp.bfloat16)
        output = jnp.dot(activated, down_weight, preferred_element_type=jnp.float32) + down_bias + wide
        slope = (jnp.dot(upstream, down_weight.T, preferred_element_type=jnp.float32) * gelu_slope(preact)).astype(jnp.bfloat16)
        down_acc = down_acc + jnp.dot(activated.T, upstream, preferred_element_type=jnp.float32)
        up_acc = up_acc + jnp.dot(normed.T, slope, preferred_element_type=jnp.float32)
        bias_acc = bias_acc + lax.optimization_barrier(jnp.sum(slope.astype(jnp.float32), axis=0))
        normed_back = jnp.dot(slope, up_weight.T, preferred_element_type=jnp.float32)
        gain_acc = gain_acc + lax.optimization_barrier(jnp.sum(normed_back * standard, axis=0))
        shift_acc = shift_acc + lax.optimization_barrier(jnp.sum(normed_back, axis=0))
        scaled = normed_back * norm_gain
        back = inverse_spread * (scaled - lax.optimization_barrier(jnp.mean(scaled, axis=1, keepdims=True)) - standard * lax.optimization_barrier(jnp.mean(scaled * standard, axis=1, keepdims=True)))
        patch_grad = back + upstream.astype(jnp.float32)
        return ((up_acc, down_acc, bias_acc, gain_acc, shift_acc), (output, patch_grad))
    start = (jnp.zeros((D, FF), jnp.float32), jnp.zeros((FF, D), jnp.float32), jnp.zeros((FF,), jnp.float32), jnp.zeros((D,), jnp.float32), jnp.zeros((D,), jnp.float32))
    sums, results = lax.scan(one_block, start, (patch_blocks, upstream_blocks))
    scaling = 1.0 / math.sqrt(TOKENS)
    output = results[0].reshape(TOKENS, D)
    patch_grad = results[1].reshape(TOKENS, D)
    norm_grad = jnp.stack([sums[3], sums[4]]) * scaling
    return (output, patch_grad, sums[0] * scaling, sums[1] * scaling, sums[2] * scaling, norm_grad)
```

```python
import math

import jax
import jax.numpy as jnp
from jax import lax
from jax.sharding import PartitionSpec as P

EPSILON = 1e-06
GELU_ROOT = 0.7978845608028654
GELU_CUBIC = 0.044715
CHUNKS = 4


def gelu_value(value):
    inner = jnp.tanh(GELU_ROOT * (value + GELU_CUBIC * value * value * value))
    return 0.5 * value * (1.0 + inner)


def gelu_slope(value):
    inner = jnp.tanh(GELU_ROOT * (value + GELU_CUBIC * value * value * value))
    return 0.5 * (1.0 + inner) + 0.5 * value * (1.0 - inner * inner) * GELU_ROOT * (
        1.0 + 3.0 * GELU_CUBIC * value * value
    )


def contract_rows(left, right):
    return lax.dot_general(
        left, right, (((0,), (0,)), ((), ())), preferred_element_type=jnp.float32
    )


def contract_cols(left, right):
    return lax.dot_general(
        left, right, (((1,), (1,)), ((), ())), preferred_element_type=jnp.float32
    )


def pair_exchange(value, axis, distance):
    size = lax.axis_size(axis)
    return lax.ppermute(value, axis, [(at, at ^ distance) for at in range(size)])


def small_total(value, axis):
    size = lax.axis_size(axis)
    if size & (size - 1):
        return lax.psum(value, axis)
    distance = 1
    while distance < size:
        value = value + pair_exchange(value, axis, distance)
        distance *= 2
    return value


def add_narrow(left, right):
    return (left.astype(jnp.float32) + right.astype(jnp.float32)).astype(jnp.bfloat16)


def line_total(value, position):
    size = lax.axis_size("dp")
    chips = size // 2

    def moves(pairs):
        return [(2 * source + core, 2 * target + core) for source, target in pairs for core in range(2)]

    inward = [
        [(step, step + 1), (chips - 1 - step, chips - 2 - step)] for step in range(chips // 2 - 1)
    ]
    for pairs in inward:
        value = add_narrow(value, lax.ppermute(value, "dp", moves(pairs)))
    middle = chips // 2
    value = add_narrow(
        value, lax.ppermute(value, "dp", moves([(middle - 1, middle), (middle, middle - 1)]))
    )
    for pairs in reversed(inward):
        arrived = lax.ppermute(value, "dp", moves([(target, source) for source, target in pairs]))
        takes = (position == pairs[0][0]) | (position == pairs[1][0])
        value = jnp.where(takes, arrived, value)
    return value


def gather_tokens(normed, cotangent):
    if lax.axis_size("row") == 2:
        over_col = [pair_exchange(one, "col", 1) for one in (cotangent, normed)]
        over_row = [pair_exchange(one, "row", 1) for one in (cotangent, normed)]
        cotangent_far = pair_exchange(over_row[0], "col", 1)
        normed_far = pair_exchange(over_col[1], "row", 1)
        return (
            jnp.concatenate([normed, over_col[1], over_row[1], normed_far], axis=0),
            jnp.concatenate([cotangent, over_col[0], over_row[0], cotangent_far], axis=0),
        )
    both = jnp.stack([normed, cotangent])
    both = lax.all_gather(both, "row", axis=1, tiled=True)
    other = pair_exchange(both, "col", 1)
    both = jnp.concatenate([both, other], axis=1)
    return both[0], both[1]


def return_tokens(partial, local_rows, side):
    half_width = partial.shape[1]
    if lax.axis_size("row") == 2:
        blocks = partial.reshape(4, local_rows, half_width)
        arrived = pair_exchange(blocks[2:].astype(jnp.bfloat16), "row", 1)
        summed = blocks[:2] + arrived.astype(jnp.float32)
    else:
        n_row = lax.axis_size("row")
        blocks = partial.reshape(2, n_row, local_rows, half_width)
        summed = lax.psum_scatter(blocks, "row", scatter_dimension=1, tiled=True)
        summed = summed.reshape(2, local_rows, half_width)
    other = pair_exchange(summed[1].astype(jnp.bfloat16), "col", 1).astype(jnp.float32)
    own = summed[0]
    return jnp.where(
        side == 0,
        jnp.concatenate([own, other], axis=1),
        jnp.concatenate([other, own], axis=1),
    )


def chunk_count(columns):
    for count in (CHUNKS, 4, 3, 2):
        if columns % (count * 256) == 0:
            return count
    return 1


def on_device(patches, norm_gain, norm_bias, up_weight, up_bias, down_weight, down_bias, cotangent):
    n_row = lax.axis_size("row")
    n_col = lax.axis_size("col")
    n_replica = lax.axis_size("dp")
    local_rows = patches.shape[0]
    width = patches.shape[1]
    half_width = width // n_col
    hidden = up_weight.shape[1]
    scaling = 1.0 / math.sqrt(local_rows * n_row * n_col * n_replica)
    side = lax.axis_index("col")
    replica = lax.axis_index("dp")
    core = replica % 2
    chip = replica // 2
    chunks = chunk_count(hidden)
    piece = hidden // (2 * chunks)

    starts = [
        [(2 * k + core) * piece for k in range(chunks)],
        [(2 * k + 1 - core) * piece for k in range(chunks)],
    ]
    up_own = [[lax.dynamic_slice_in_dim(up_weight, at, piece, 1) for at in part] for part in starts]
    down_own = [[lax.dynamic_slice_in_dim(down_weight, at, piece, 0) for at in part] for part in starts]
    bias_own = [[lax.dynamic_slice_in_dim(up_bias, at, piece, 0) for at in part] for part in starts]

    wide_patches = patches.astype(jnp.float32)
    centred = wide_patches - jnp.mean(wide_patches, axis=1, keepdims=True)
    inverse_spread = lax.rsqrt(jnp.mean(centred * centred, axis=1, keepdims=True) + EPSILON)
    standard = centred * inverse_spread
    normed = (standard * norm_gain + norm_bias).astype(jnp.bfloat16)
    normed_all, upstream = gather_tokens(normed, cotangent)
    normed_near = lax.dynamic_slice_in_dim(normed_all, side * half_width, half_width, 1)
    normed_away = lax.dynamic_slice_in_dim(normed_all, (1 - side) * half_width, half_width, 1)
    upstream_near = lax.dynamic_slice_in_dim(upstream, side * half_width, half_width, 1)
    upstream_away = lax.dynamic_slice_in_dim(upstream, (1 - side) * half_width, half_width, 1)

    activated_parts, slope_parts, bias_parts = [], [], [[], []]
    up_parts, down_parts = [], []
    for k in range(chunks):
        up_first = pair_exchange(up_own[0][k], "col", 1)
        down_first = pair_exchange(down_own[0][k], "col", 1)
        up_other = [up_first, pair_exchange(up_first, "dp", 1)]
        down_other = [down_first, pair_exchange(down_first, "dp", 1)]
        up_pair, down_pair = [], []
        for part in range(2):
            preact = (
                jnp.dot(normed_near, up_own[part][k], preferred_element_type=jnp.float32)
                + jnp.dot(normed_away, up_other[part], preferred_element_type=jnp.float32)
                + bias_own[part][k]
            )
            activated = gelu_value(preact).astype(jnp.bfloat16)
            slope = (
                (
                    contract_cols(upstream_near, down_own[part][k])
                    + contract_cols(upstream_away, down_other[part])
                )
                * gelu_slope(preact)
            ).astype(jnp.bfloat16)
            activated_parts.append((activated, down_own[part][k]))
            slope_parts.append((slope, up_own[part][k]))
            bias_parts[part].append(jnp.sum(slope.astype(jnp.float32), axis=0))
            up_pair.append((contract_rows(normed_near, slope) * scaling))
            down_pair.append((contract_rows(activated, upstream_near) * scaling))
        up_sum = add_narrow(up_pair[0], pair_exchange(up_pair[1].astype(jnp.bfloat16), "dp", 1))
        down_sum = add_narrow(down_pair[0], pair_exchange(down_pair[1].astype(jnp.bfloat16), "dp", 1))
        up_sum = line_total(up_sum, chip)
        down_sum = line_total(down_sum, chip)
        up_pieces = [up_sum, pair_exchange(up_sum, "dp", 1)]
        down_pieces = [down_sum, pair_exchange(down_sum, "dp", 1)]
        for near, away in ((0, 1), (1, 0)):
            up_parts.append(jnp.where(core == 0, up_pieces[near], up_pieces[away]).astype(jnp.float32))
            down_parts.append(jnp.where(core == 0, down_pieces[near], down_pieces[away]).astype(jnp.float32))
    up_grad = jnp.concatenate(up_parts, axis=1)
    down_grad = jnp.concatenate(down_parts, axis=0)

    projected = jnp.dot(
        jnp.concatenate([one for one, _ in activated_parts], axis=1),
        jnp.concatenate([one for _, one in activated_parts], axis=0),
        preferred_element_type=jnp.float32,
    )
    output = return_tokens(projected, local_rows, side) + down_bias + wide_patches
    partial_back = contract_cols(
        jnp.concatenate([one for one, _ in slope_parts], axis=1),
        jnp.concatenate([one for _, one in slope_parts], axis=1),
    )
    normed_back = return_tokens(partial_back, local_rows, side)
    norm_terms = jnp.concatenate([jnp.sum(normed_back * standard, axis=0), jnp.sum(normed_back, axis=0)])
    norm_terms = small_total(small_total(norm_terms, "row"), "col")
    bias_sums = []
    for k in range(chunks):
        for near, away in ((0, 1), (1, 0)):
            bias_sums.append(jnp.where(core == 0, bias_parts[near][k], bias_parts[away][k]))
    totals = small_total(jnp.concatenate(bias_sums + [norm_terms]), "dp") * scaling
    scaled = normed_back * norm_gain
    back = inverse_spread * (
        scaled
        - jnp.mean(scaled, axis=1, keepdims=True)
        - standard * jnp.mean(scaled * standard, axis=1, keepdims=True)
    )
    patch_grad = back + cotangent.astype(jnp.float32)
    return (
        output,
        patch_grad,
        up_grad,
        down_grad,
        totals[:hidden],
        totals[hidden:].reshape(2, width),
    )


def solution(mesh):
    in_specs = (
        P(("dp", "row", "col"), None),
        P(),
        P(),
        P("col", "row"),
        P("row"),
        P("row", "col"),
        P(),
        P(("dp", "row", "col"), None),
    )
    out_specs = (
        P(("dp", "row", "col"), None),
        P(("dp", "row", "col"), None),
        P("col", "row"),
        P("row", "col"),
        P("row"),
        P(),
    )
    return jax.shard_map(
        on_device, mesh=mesh, in_specs=in_specs, out_specs=out_specs, check_vma=False
    )
```

```python
import functools
import math

import jax
import jax.numpy as jnp
from jax import lax
from jax.experimental import pallas as pl
from jax.experimental.pallas import tpu as pltpu
from jax.sharding import PartitionSpec as P

EPSILON = 1e-06
GELU_ROOT = 0.7978845608028654
GELU_CUBIC = 0.044715


def gelu_value(value):
    inner = jnp.tanh(GELU_ROOT * (value + GELU_CUBIC * value * value * value))
    return 0.5 * value * (1.0 + inner)


def gelu_slope(value):
    inner = jnp.tanh(GELU_ROOT * (value + GELU_CUBIC * value * value * value))
    return 0.5 * (1.0 + inner) + 0.5 * value * (1.0 - inner * inner) * GELU_ROOT * (
        1.0 + 3.0 * GELU_CUBIC * value * value
    )


def contract_rows(left, right):
    return lax.dot_general(
        left, right, (((0,), (0,)), ((), ())), preferred_element_type=jnp.float32
    )


def contract_cols(left, right):
    return lax.dot_general(
        left, right, (((1,), (1,)), ((), ())), preferred_element_type=jnp.float32
    )


def pair_exchange(value, axis, distance):
    size = lax.axis_size(axis)
    return lax.ppermute(value, axis, [(at, at ^ distance) for at in range(size)])


def small_total(value, axis):
    size = lax.axis_size(axis)
    if size & (size - 1):
        return lax.psum(value, axis)
    distance = 1
    while distance < size:
        value = value + pair_exchange(value, axis, distance)
        distance *= 2
    return value


def line_kernel(
    chips, rows, given, total, from_core, held, from_outer, from_middle,
    core_send, core_recv, in_send, outer_recv, middle_recv, out_send, out_recv, share_send, share_recv,
):
    steps = given.shape[1] // rows
    replica = lax.axis_index("dp")
    core = lax.rem(replica, 2)
    chip = replica // 2
    upper = chip // (chips // 2)
    inner = chip + 1 - 2 * upper
    outer = chip - 1 + 2 * upper
    depth = chip + upper * (chips - 1 - 2 * chip)
    is_end = depth == 0
    is_middle = depth == chips // 2 - 1
    partner_id = {"dp": replica + 1 - 2 * core}
    inner_id = {"dp": 2 * inner + core}
    outer_id = {"dp": 2 * outer + core}

    def remote(source, target, send, recv, device):
        return pltpu.make_async_remote_copy(
            src_ref=source, dst_ref=target, send_sem=send, recv_sem=recv,
            device_id=device, device_id_type=pl.DeviceIdType.MESH,
        )

    def span(k):
        return pl.ds(pl.multiple_of(k * rows, rows), rows)

    def core_copy(k):
        return remote(
            given.at[1 - core, span(k)], from_core.at[span(k)], core_send.at[k], core_recv.at[k], partner_id
        )

    def inward_copy(k):
        return remote(held.at[span(k)], from_outer.at[span(k)], in_send.at[k], outer_recv.at[k], inner_id)

    def middle_copy(k):
        return remote(held.at[span(k)], from_middle.at[span(k)], in_send.at[k], middle_recv.at[k], inner_id)

    def outward_copy(k):
        return remote(
            total.at[core, span(k)], total.at[core, span(k)], out_send.at[k], out_recv.at[k], outer_id
        )

    def share_copy(k, kind):
        return remote(
            total.at[kind, span(k)], total.at[kind, span(k)], share_send.at[k], share_recv.at[k], partner_id
        )

    barrier = pltpu.get_barrier_semaphore()
    pl.semaphore_signal(barrier, inc=1, device_id=partner_id, device_id_type=pl.DeviceIdType.MESH)
    pl.semaphore_signal(barrier, inc=1, device_id=inner_id, device_id_type=pl.DeviceIdType.MESH)

    @pl.when(jnp.logical_not(is_end))
    def _():
        pl.semaphore_signal(barrier, inc=1, device_id=outer_id, device_id_type=pl.DeviceIdType.MESH)
        pl.semaphore_wait(barrier, 3)

    @pl.when(is_end)
    def _():
        pl.semaphore_wait(barrier, 2)

    def each(body):
        def step(k, carry):
            body(k)
            return carry

        lax.fori_loop(0, steps, step, 0)

    each(lambda k: core_copy(k).start())

    def inward(k):
        core_copy(k).wait_recv()
        summed = given[core, span(k)].astype(jnp.float32) + from_core[span(k)].astype(jnp.float32)
        held[span(k)] = summed.astype(jnp.bfloat16)

        @pl.when(jnp.logical_not(is_end))
        def _():
            inward_copy(k).wait_recv()
            held[span(k)] = (
                held[span(k)].astype(jnp.float32) + from_outer[span(k)].astype(jnp.float32)
            ).astype(jnp.bfloat16)

        @pl.when(is_middle)
        def _():
            middle_copy(k).start()

        @pl.when(jnp.logical_not(is_middle))
        def _():
            inward_copy(k).start()

    def outward(k):
        @pl.when(is_middle)
        def _():
            middle_copy(k).wait_recv()
            total[core, span(k)] = (
                held[span(k)].astype(jnp.float32) + from_middle[span(k)].astype(jnp.float32)
            ).astype(jnp.bfloat16)

        @pl.when(jnp.logical_not(is_middle))
        def _():
            outward_copy(k).wait_recv()

        @pl.when(jnp.logical_not(is_end))
        def _():
            outward_copy(k).start()

        share_copy(k, core).start()

    @pl.when(is_end)
    def _():
        each(inward)
        each(outward)

    @pl.when(jnp.logical_not(is_end))
    def _():
        inward(0)
        inward(1)

        def step(k, carry):
            inward(k)
            outward(k - 2)
            return carry

        lax.fori_loop(2, steps, step, 0)
        outward(steps - 2)
        outward(steps - 1)

    def finish(k):
        core_copy(k).wait_send()
        inward_copy(k).wait_send()

        @pl.when(jnp.logical_not(is_end))
        def _():
            outward_copy(k).wait_send()

        share_copy(k, core).wait_send()
        share_copy(k, 1 - core).wait_recv()

    each(finish)


def replica_total(grads):
    chips = lax.axis_size("dp") // 2
    kinds, height, columns = grads.shape
    rows = 32
    steps = height // rows
    slot = pltpu.VMEM((height, columns), jnp.bfloat16)
    return pl.pallas_call(
        functools.partial(line_kernel, chips, rows),
        out_shape=jax.ShapeDtypeStruct(grads.shape, jnp.bfloat16),
        in_specs=[pl.BlockSpec(memory_space=pltpu.VMEM)],
        out_specs=pl.BlockSpec(memory_space=pltpu.VMEM),
        scratch_shapes=[slot] * 4 + [pltpu.SemaphoreType.DMA((steps,))] * 9,
        compiler_params=pltpu.CompilerParams(
            collective_id=0, has_side_effects=True, vmem_limit_bytes=48 * 1024 * 1024
        ),
        cost_estimate=pl.CostEstimate(flops=0, bytes_accessed=400 * 1024 * 1024, transcendentals=0),
    )(grads)


def gather_tokens(normed, cotangent):
    if lax.axis_size("row") == 2:
        over_col = [pair_exchange(one, "col", 1) for one in (cotangent, normed)]
        over_row = [pair_exchange(one, "row", 1) for one in (cotangent, normed)]
        cotangent_far = pair_exchange(over_row[0], "col", 1)
        normed_far = pair_exchange(over_col[1], "row", 1)
        return (
            jnp.concatenate([normed, over_col[1], over_row[1], normed_far], axis=0),
            jnp.concatenate([cotangent, over_col[0], over_row[0], cotangent_far], axis=0),
        )
    both = jnp.stack([normed, cotangent])
    both = lax.all_gather(both, "row", axis=1, tiled=True)
    other = pair_exchange(both, "col", 1)
    both = jnp.concatenate([both, other], axis=1)
    return both[0], both[1]


def return_tokens(partial, local_rows, side):
    half_width = partial.shape[1]
    if lax.axis_size("row") == 2:
        blocks = partial.reshape(4, local_rows, half_width)
        arrived = pair_exchange(blocks[2:].astype(jnp.bfloat16), "row", 1)
        summed = blocks[:2] + arrived.astype(jnp.float32)
    else:
        n_row = lax.axis_size("row")
        blocks = partial.reshape(2, n_row, local_rows, half_width)
        summed = lax.psum_scatter(blocks, "row", scatter_dimension=1, tiled=True)
        summed = summed.reshape(2, local_rows, half_width)
    other = pair_exchange(summed[1].astype(jnp.bfloat16), "col", 1).astype(jnp.float32)
    own = summed[0]
    return jnp.where(
        side == 0,
        jnp.concatenate([own, other], axis=1),
        jnp.concatenate([other, own], axis=1),
    )


def on_device(patches, norm_gain, norm_bias, up_weight, up_bias, down_weight, down_bias, cotangent):
    n_row = lax.axis_size("row")
    n_col = lax.axis_size("col")
    n_replica = lax.axis_size("dp")
    local_rows = patches.shape[0]
    width = patches.shape[1]
    half_width = width // n_col
    hidden = up_weight.shape[1]
    scaling = 1.0 / math.sqrt(local_rows * n_row * n_col * n_replica)
    side = lax.axis_index("col")
    replica = lax.axis_index("dp")
    core = replica % 2
    piece = hidden // 2

    up_first = pair_exchange(lax.dynamic_slice_in_dim(up_weight, core * piece, piece, 1), "col", 1)
    down_first = pair_exchange(lax.dynamic_slice_in_dim(down_weight, core * piece, piece, 0), "col", 1)
    up_second = pair_exchange(up_first, "dp", 1)
    down_second = pair_exchange(down_first, "dp", 1)
    up_other = jnp.where(
        core == 0,
        jnp.concatenate([up_first, up_second], axis=1),
        jnp.concatenate([up_second, up_first], axis=1),
    )
    down_other = jnp.where(
        core == 0,
        jnp.concatenate([down_first, down_second], axis=0),
        jnp.concatenate([down_second, down_first], axis=0),
    )

    wide_patches = patches.astype(jnp.float32)
    centred = wide_patches - jnp.mean(wide_patches, axis=1, keepdims=True)
    inverse_spread = lax.rsqrt(jnp.mean(centred * centred, axis=1, keepdims=True) + EPSILON)
    standard = centred * inverse_spread
    normed = (standard * norm_gain + norm_bias).astype(jnp.bfloat16)
    normed_all, upstream = gather_tokens(normed, cotangent)
    normed_near = lax.dynamic_slice_in_dim(normed_all, side * half_width, half_width, 1)
    normed_away = lax.dynamic_slice_in_dim(normed_all, (1 - side) * half_width, half_width, 1)
    upstream_near = lax.dynamic_slice_in_dim(upstream, side * half_width, half_width, 1)
    upstream_away = lax.dynamic_slice_in_dim(upstream, (1 - side) * half_width, half_width, 1)

    preact = (
        jnp.dot(normed_near, up_weight, preferred_element_type=jnp.float32)
        + jnp.dot(normed_away, up_other, preferred_element_type=jnp.float32)
        + up_bias
    )
    activated = gelu_value(preact).astype(jnp.bfloat16)
    slope = (
        (contract_cols(upstream_near, down_weight) + contract_cols(upstream_away, down_other))
        * gelu_slope(preact)
    ).astype(jnp.bfloat16)
    grads = jnp.stack(
        [
            (contract_rows(normed_near, slope) * scaling).astype(jnp.bfloat16),
            (contract_rows(upstream_near, activated) * scaling).astype(jnp.bfloat16),
        ]
    )
    totals_wide = replica_total(grads)
    up_grad = totals_wide[0].astype(jnp.float32)
    down_grad = totals_wide[1].T.astype(jnp.float32)

    projected = jnp.dot(activated, down_weight, preferred_element_type=jnp.float32)
    output = return_tokens(projected, local_rows, side) + down_bias + wide_patches
    partial_back = contract_cols(slope, up_weight)
    normed_back = return_tokens(partial_back, local_rows, side)
    norm_terms = jnp.concatenate([jnp.sum(normed_back * standard, axis=0), jnp.sum(normed_back, axis=0)])
    norm_terms = small_total(small_total(norm_terms, "row"), "col")
    bias_terms = jnp.sum(slope.astype(jnp.float32), axis=0)
    totals = small_total(jnp.concatenate([bias_terms, norm_terms]), "dp") * scaling
    scaled = normed_back * norm_gain
    back = inverse_spread * (
        scaled
        - jnp.mean(scaled, axis=1, keepdims=True)
        - standard * jnp.mean(scaled * standard, axis=1, keepdims=True)
    )
    patch_grad = back + cotangent.astype(jnp.float32)
    return (
        output,
        patch_grad,
        up_grad,
        down_grad,
        totals[:hidden],
        totals[hidden:].reshape(2, width),
    )


def solution(mesh):
    in_specs = (
        P(("dp", "row", "col"), None),
        P(),
        P(),
        P("col", "row"),
        P("row"),
        P("row", "col"),
        P(),
        P(("dp", "row", "col"), None),
    )
    out_specs = (
        P(("dp", "row", "col"), None),
        P(("dp", "row", "col"), None),
        P("col", "row"),
        P("row", "col"),
        P("row"),
        P(),
    )
    return jax.shard_map(
        on_device, mesh=mesh, in_specs=in_specs, out_specs=out_specs, check_vma=False
    )
```
